32 devices in a mesh: grp: 2 (over y), vec: 4 (over z), occ: 2 (over x), wlk: 2 (over core).
Axes of the slice: x: 2, y: 2, z: 4, core: 2. Of those that a mesh axis runs over, the one named last changes fastest.
Arguments:
- chol_half: bfloat16 [256, 256, 2048], P(('grp', 'vec'), 'occ'), parts along dimension 0, may hold values from -0.046875 to 0.046875
- theta: bfloat16 [8, 2048, 256], P(('grp', 'wlk'), 'vec', 'occ'), parts along dimension 0, may hold values from -6 to 6
Outputs:
- theta_grad: float32 [8, 2048, 256], P(('grp', 'wlk'), 'vec', 'occ'), parts along dimension 0
The draws below stay inside these ranges and needn't reach their ends.
There are 2 independent parts, one for each index of `grp`. The reference program is written for one: setup_inputs(seed, part) draws one part's arguments, and reference() takes and returns one part's arrays. A program takes and returns all parts, laid end to end along the dimension named above; each array names one. Nothing has to cross between parts.
All inputs are finite; a program needn't handle non-finite values.
Results may differ from the reference program's by a relative error of at most 0.0042.
Values may be sent and summed in bfloat16 or wider, within the bound.
A program may use at most 64 MiB of HBM per device.

```python
import jax
import jax.numpy as jnp
from jax import lax

M = 2048
O = 256
NCHOL = 128
W = 4


def steps_of(own_key, shape, cuts, least, largest):
    loudness, own = 1.0, jax.random.fold_in(own_key, 6)
    for axis_at, shards_of in cuts:
        steps = jnp.exp(jax.random.uniform(jax.random.fold_in(own, axis_at), (shards_of,), jnp.float32, least / len(cuts), largest / len(cuts)))
        loudness = loudness * jnp.repeat(steps, shape[axis_at] // shards_of).reshape([-1 if axis == axis_at else 1 for axis in range(len(shape))])
    return loudness


def scatter_about(rng, shape, scale, reach, shards=(), kind=jnp.bfloat16):
    loudness = steps_of(rng, shape, shards, -0.22, 0.18) if shards else 1.0
    drawn = jax.random.normal(rng, shape, jnp.float32) * scale * loudness
    return jnp.minimum(jnp.maximum(drawn, -reach), reach).astype(kind)


def setup_inputs(seed: int = 0, part: int = 0) -> dict:
    key_list = jax.random.split(jax.random.key(seed), 3)
    own_keys = jax.random.split(jax.random.fold_in(key_list[2], part), 3)
    return {
        "chol_half": scatter_about(own_keys[0], (NCHOL, O, M), (7 * M) ** -0.5, 0.046875, ((0, 4), (1, 2))),
        "theta": scatter_about(own_keys[1], (W, M, O), 1.0, 6.0, ((0, 2), (1, 4), (2, 2))),
    }


def reference(chol_half, theta):
    walkers = theta.shape[0]

    def add_vector(carry, factor):
        grads = []
        for walker in range(walkers):
            amplitudes = jnp.dot(factor, theta[walker], preferred_element_type=jnp.float32).astype(jnp.bfloat16)
            grads.append(jnp.dot(factor.T, amplitudes.T, preferred_element_type=jnp.float32))
        return carry + jnp.stack(grads), None

    initial = jnp.zeros((walkers, M, O), jnp.float32)
    total, unused = lax.scan(add_vector, initial, chol_half)
    return -total
```

```python
import functools

import jax
import jax.numpy as jnp
from jax import lax
from jax.experimental import pallas as pl
from jax.experimental.pallas import tpu as pltpu
from jax.sharding import PartitionSpec as P

MESH = pl.DeviceIdType.MESH
F32 = jnp.float32
BF16 = jnp.bfloat16


def kernel(nz, dims, chol, theta, out, cv, thp, thd, asend, arecv, adiag, accd, accr, gsend, grecv, gown, xs, xr,
           csem, txs, txr, tzs, tzr, ass, asr, gss, gsr, xss, xsr):
    G, R, M, W, Q, CH = dims
    GC = G // CH
    z = lax.axis_index("vec")
    partner = {"occ": 1 - lax.axis_index("occ")}
    peers = [lax.rem(z + k, nz) for k in range(1, nz)]
    mine = pl.ds(pl.multiple_of(z * Q, Q), Q)

    def c_copy(c):
        part = pl.ds(c * GC, GC)
        return pltpu.make_async_copy(chol.at[part], cv.at[part], csem.at[c])

    def remote(src, dst, ss, rs, to):
        return pltpu.make_async_remote_copy(src_ref=src, dst_ref=dst, send_sem=ss, recv_sem=rs, device_id=to, device_id_type=MESH)

    for c in range(CH):
        c_copy(c).start()

    barrier = pltpu.get_barrier_semaphore()
    pl.semaphore_signal(barrier, inc=1, device_id=partner, device_id_type=MESH)
    for peer in peers:
        pl.semaphore_signal(barrier, inc=1, device_id={"vec": peer}, device_id_type=MESH)
    pl.semaphore_wait(barrier, nz)

    def theta_x(w):
        return remote(theta.at[w], thp.at[w, mine], txs.at[w], txr.at[w], partner)

    def rows_of(s):
        return pl.ds(pl.multiple_of(s * Q, Q), Q)

    def theta_p(w, k, s):
        rows = rows_of(s)
        return remote(thp.at[w, rows], thp.at[w, rows], tzs.at[w, k], tzr.at[w, s], {"vec": peers[k]})

    def theta_d(w, k, s):
        return remote(theta.at[w], thd.at[rows_of(s), pl.ds(w * R, R)], tzs.at[W + w, k], tzr.at[W + w, s], {"vec": peers[k]})

    for w in range(W):
        theta_x(w).start()
    for w in range(W):
        theta_x(w).wait_recv()
        for k in range(nz - 1):
            theta_p(w, k, z).start()
    for w in range(W):
        for k in range(nz - 1):
            theta_d(w, k, z).start()
        thd[mine, pl.ds(w * R, R)] = theta[w]

    def a_copy(w, c):
        part = pl.ds(c * GC, GC)
        return remote(asend.at[w, part], arecv.at[w, part], ass.at[w, c], asr.at[w, c], partner)

    for w in range(W):
        for k in range(nz - 1):
            theta_p(w, k, peers[k]).wait_recv()

        @pl.loop(0, CH)
        def _(c):
            if w == 0:
                c_copy(c).wait()
            part = pl.ds(c * GC, GC)
            block = jnp.dot(cv[part].reshape(GC * R, M), thp[w], preferred_element_type=F32)
            asend[w, part] = block.astype(BF16).reshape(GC, R, R)
            a_copy(w, c).start()

    def g_copy(e, k, s, d):
        return remote(gsend.at[e, d], grecv.at[e, s], gss.at[e, k], gsr.at[e, s], {"vec": peers[k]})

    def scatter(e, acc, first):
        rows = pl.ds(first, R)
        for d in range(nz):
            gsend[e, d] = acc[rows, pl.ds(d * Q, Q)].astype(BF16)
        gown[e] = acc[rows, mine]
        for k in range(nz - 1):
            g_copy(e, k, z, peers[k]).start()

    def gathered(e):
        total = gown[e]
        for k in range(nz - 1):
            g_copy(e, k, peers[k], peers[k]).wait_recv()
            total = total + grecv[e, peers[k]].astype(F32)
        return total

    def x_copy(w):
        return remote(xs.at[w], xr.at[w], xss.at[w], xsr.at[w], partner)

    for w in range(W):
        for k in range(nz - 1):
            theta_d(w, k, peers[k]).wait_recv()
    accd[...] = jnp.zeros_like(accd)

    @pl.loop(0, CH)
    def _(c):
        part = pl.ds(c * GC, GC)
        block = jnp.dot(cv[part].reshape(GC * R, M), thd[...], preferred_element_type=F32)
        adiag[part] = block.astype(BF16).reshape(GC, R, W * R)

    def add_chunk(acc, lhs, part):
        for n in range(nz):
            cols = pl.ds(n * Q, Q)
            acc[:, cols] += jnp.dot(lhs, cv[part, :, cols].reshape(GC * R, Q), preferred_element_type=F32)

    @pl.loop(0, CH)
    def _(c):
        part = pl.ds(c * GC, GC)
        block = adiag[part]
        lhs = jnp.concatenate(
            [jnp.concatenate([block[g, :, w * R:(w + 1) * R] for g in range(GC)], axis=1) for w in range(W)], axis=0
        )
        add_chunk(accd, lhs, part)

    for w in range(W):
        if w == 0:
            for v in range(W):
                scatter(v, accd, v * R)
        accr[...] = jnp.zeros_like(accr)

        @pl.loop(0, CH)
        def _(c):
            a_copy(w, c).wait_recv()
            part = pl.ds(c * GC, GC)
            block = arecv[w, part]
            add_chunk(accr, jnp.concatenate([block[g] for g in range(GC)], axis=1), part)

        scatter(W + w, accr, 0)

    for w in range(W):
        gown[w] = gathered(w)
    for w in range(W):
        xs[w] = gathered(W + w).astype(BF16)
        x_copy(w).start()
    for w in range(W):
        x_copy(w).wait_recv()
        out[w] = -(gown[w] + xr[w].astype(F32)).T

    for w in range(W):
        theta_x(w).wait_send()
        x_copy(w).wait_send()
        for k in range(nz - 1):
            theta_p(w, k, z).wait_send()
            theta_d(w, k, z).wait_send()
            g_copy(w, k, z, peers[k]).wait_send()
            g_copy(W + w, k, z, peers[k]).wait_send()

        @pl.loop(0, CH)
        def _(c):
            a_copy(w, c).wait_send()


def fused(nz, chol_half, theta):
    G, R, M = chol_half.shape
    W, Q, _ = theta.shape
    CH = 8 if G % 8 == 0 else 1
    dims = (G, R, M, W, Q, CH)
    dma = pltpu.SemaphoreType.DMA
    return pl.pallas_call(
        functools.partial(kernel, nz, dims),
        out_shape=jax.ShapeDtypeStruct((W, Q, R), F32),
        in_specs=[pl.BlockSpec(memory_space=pl.ANY), pl.BlockSpec(memory_space=pltpu.VMEM)],
        out_specs=pl.BlockSpec(memory_space=pltpu.VMEM),
        scratch_shapes=[
            pltpu.VMEM((G, R, M), BF16),
            pltpu.VMEM((W, M, R), BF16),
            pltpu.VMEM((M, W * R), BF16),
            pltpu.VMEM((W, G, R, R), BF16),
            pltpu.VMEM((W, G, R, R), BF16),
            pltpu.VMEM((G, R, W * R), BF16),
            pltpu.VMEM((W * R, M), F32),
            pltpu.VMEM((R, M), F32),
            pltpu.VMEM((2 * W, nz, R, Q), BF16),
            pltpu.VMEM((2 * W, nz, R, Q), BF16),
            pltpu.VMEM((2 * W, R, Q), F32),
            pltpu.VMEM((W, R, Q), BF16),
            pltpu.VMEM((W, R, Q), BF16),
            dma((CH,)),
            dma((W,)),
            dma((W,)),
            dma((2 * W, nz)),
            dma((2 * W, nz)),
            dma((W, CH)),
            dma((W, CH)),
            dma((2 * W, nz)),
            dma((2 * W, nz)),
            dma((W,)),
            dma((W,)),
        ],
        compiler_params=pltpu.CompilerParams(collective_id=0, has_side_effects=True, vmem_limit_bytes=60 << 20),
    )(chol_half, theta)


def on_device(mesh, chol_half, theta):
    G, R, M = chol_half.shape
    nz = mesh.shape["vec"]
    if mesh.shape["occ"] == 2 and R % 128 == 0 and theta.shape[1] % 128 == 0 and G * R * M <= 8 << 20:
        return fused(nz, chol_half, theta)
    widened = lax.all_gather(theta, "occ", axis=2, tiled=True)
    amplitude_sums = jnp.einsum(
        "gip,wpj->wgij", chol_half, lax.all_gather(widened, "vec", axis=1, tiled=True), preferred_element_type=F32
    )
    amplitudes = amplitude_sums.astype(BF16)
    swapped = lax.all_to_all(amplitudes, "occ", split_axis=3, concat_axis=2, tiled=True)
    summed_rows = lax.psum_scatter(
        jnp.einsum("gap,wgba->pwb", chol_half, swapped, preferred_element_type=F32),
        "vec",
        scatter_dimension=0,
        tiled=True,
    )
    owned = lax.psum_scatter(summed_rows, "occ", scatter_dimension=2, tiled=True)
    return -jnp.transpose(owned, (1, 0, 2))


def solution(mesh):
    return jax.shard_map(
        functools.partial(on_device, mesh),
        mesh=mesh,
        in_specs=(P(("grp", "vec"), "occ", None), P(("grp", "wlk"), "vec", "occ")),
        out_specs=P(("grp", "wlk"), "vec", "occ"),
        check_vma=False,
    )
```

```python
import functools

import jax
import jax.numpy as jnp
from jax import lax
from jax.experimental import pallas as pl
from jax.experimental.pallas import tpu as pltpu
from jax.sharding import PartitionSpec as P

MESH = pl.DeviceIdType.MESH
F32 = jnp.float32
BF16 = jnp.bfloat16


def kernel(nz, dims, chol, theta, out, cv, thp, thd, asend, arecv, adiag, accd, accr, gsend, grecv, gown, xs, xr,
           csem, txs, txr, tzs, tzr, ass, asr, gss, gsr, xss, xsr):
    G, R, M, W, Q, CH = dims
    GC = G // CH
    z = lax.axis_index("vec")
    partner = {"occ": 1 - lax.axis_index("occ")}
    peers = [lax.rem(z + k, nz) for k in range(1, nz)]
    mine = pl.ds(pl.multiple_of(z * Q, Q), Q)

    def c_copy(c):
        part = pl.ds(c * GC, GC)
        return pltpu.make_async_copy(chol.at[part], cv.at[part], csem.at[c])

    def remote(src, dst, ss, rs, to):
        return pltpu.make_async_remote_copy(src_ref=src, dst_ref=dst, send_sem=ss, recv_sem=rs, device_id=to, device_id_type=MESH)

    for c in range(CH):
        c_copy(c).start()

    barrier = pltpu.get_barrier_semaphore()
    pl.semaphore_signal(barrier, inc=1, device_id=partner, device_id_type=MESH)
    for peer in peers:
        pl.semaphore_signal(barrier, inc=1, device_id={"vec": peer}, device_id_type=MESH)
    pl.semaphore_wait(barrier, nz)

    def theta_x(w):
        return remote(theta.at[w], thp.at[w, mine], txs.at[w], txr.at[w], partner)

    def rows_of(s):
        return pl.ds(pl.multiple_of(s * Q, Q), Q)

    def theta_p(w, k, s):
        rows = rows_of(s)
        return remote(thp.at[w, rows], thp.at[w, rows], tzs.at[w, k], tzr.at[w, s], {"vec": peers[k]})

    def theta_d(w, k, s):
        return remote(theta.at[w], thd.at[rows_of(s), pl.ds(w * R, R)], tzs.at[W + w, k], tzr.at[W + w, s], {"vec": peers[k]})

    for w in range(W):
        theta_x(w).start()
    for w in range(W):
        theta_x(w).wait_recv()
        for k in range(nz - 1):
            theta_p(w, k, z).start()
    for w in range(W):
        for k in range(nz - 1):
            theta_d(w, k, z).start()
        thd[mine, pl.ds(w * R, R)] = theta[w]

    def a_copy(w, c):
        part = pl.ds(c * GC, GC)
        return remote(asend.at[w, part], arecv.at[w, part], ass.at[w, c], asr.at[w, c], partner)

    for w in range(W):
        for k in range(nz - 1):
            theta_p(w, k, peers[k]).wait_recv()

        @pl.loop(0, CH)
        def _(c):
            if w == 0:
                c_copy(c).wait()
            part = pl.ds(c * GC, GC)
            block = jnp.dot(cv[part].reshape(GC * R, M), thp[w], preferred_element_type=F32)
            asend[w, part] = block.astype(BF16).reshape(GC, R, R)
            a_copy(w, c).start()

    def g_copy(e, k, s, d):
        return remote(gsend.at[e, d], grecv.at[e, s], gss.at[e, k], gsr.at[e, s], {"vec": peers[k]})

    def scatter(e, acc, first):
        rows = pl.ds(first, R)
        for d in range(nz):
            gsend[e, d] = acc[rows, pl.ds(d * Q, Q)].astype(BF16)
        gown[e] = acc[rows, mine]
        for k in range(nz - 1):
            g_copy(e, k, z, peers[k]).start()

    def gathered(e):
        total = gown[e]
        for k in range(nz - 1):
            g_copy(e, k, peers[k], peers[k]).wait_recv()
            total = total + grecv[e, peers[k]].astype(F32)
        return total

    def x_copy(w):
        return remote(xs.at[w], xr.at[w], xss.at[w], xsr.at[w], partner)

    def add_chunk(acc, lhs, part):
        for n in range(nz):
            cols = pl.ds(n * Q, Q)
            acc[:, cols] += jnp.dot(lhs, cv[part, :, cols].reshape(GC * R, Q), preferred_element_type=F32)

    def received(w):
        accr[...] = jnp.zeros_like(accr)

        @pl.loop(0, CH)
        def _(c):
            a_copy(w, c).wait_recv()
            part = pl.ds(c * GC, GC)
            block = arecv[w, part]
            add_chunk(accr, jnp.concatenate([block[g] for g in range(GC)], axis=1), part)

        scatter(W + w, accr, 0)

    received(0)
    for w in range(W):
        for k in range(nz - 1):
            theta_d(w, k, peers[k]).wait_recv()
    accd[...] = jnp.zeros_like(accd)

    @pl.loop(0, CH)
    def _(c):
        part = pl.ds(c * GC, GC)
        block = jnp.dot(cv[part].reshape(GC * R, M), thd[...], preferred_element_type=F32)
        adiag[part] = block.astype(BF16).reshape(GC, R, W * R)

    @pl.loop(0, CH)
    def _(c):
        part = pl.ds(c * GC, GC)
        block = adiag[part]
        lhs = jnp.concatenate(
            [jnp.concatenate([block[g, :, w * R:(w + 1) * R] for g in range(GC)], axis=1) for w in range(W)], axis=0
        )
        add_chunk(accd, lhs, part)

    for w in range(W):
        scatter(w, accd, w * R)
        if w + 1 < W:
            received(w + 1)

    for w in range(W):
        xs[w] = gathered(W + w).astype(BF16)
        x_copy(w).start()
    for w in range(W):
        gown[w] = gathered(w)
    for w in range(W):
        x_copy(w).wait_recv()
        out[w] = -(gown[w] + xr[w].astype(F32)).T

    for w in range(W):
        theta_x(w).wait_send()
        x_copy(w).wait_send()
        for k in range(nz - 1):
            theta_p(w, k, z).wait_send()
            theta_d(w, k, z).wait_send()
            g_copy(w, k, z, peers[k]).wait_send()
            g_copy(W + w, k, z, peers[k]).wait_send()

        @pl.loop(0, CH)
        def _(c):
            a_copy(w, c).wait_send()


def fused(nz, chol_half, theta):
    G, R, M = chol_half.shape
    W, Q, _ = theta.shape
    CH = 8 if G % 8 == 0 else 1
    dims = (G, R, M, W, Q, CH)
    dma = pltpu.SemaphoreType.DMA
    return pl.pallas_call(
        functools.partial(kernel, nz, dims),
        out_shape=jax.ShapeDtypeStruct((W, Q, R), F32),
        in_specs=[pl.BlockSpec(memory_space=pl.ANY), pl.BlockSpec(memory_space=pltpu.VMEM)],
        out_specs=pl.BlockSpec(memory_space=pltpu.VMEM),
        scratch_shapes=[
            pltpu.VMEM((G, R, M), BF16),
            pltpu.VMEM((W, M, R), BF16),
            pltpu.VMEM((M, W * R), BF16),
            pltpu.VMEM((W, G, R, R), BF16),
            pltpu.VMEM((W, G, R, R), BF16),
            pltpu.VMEM((G, R, W * R), BF16),
            pltpu.VMEM((W * R, M), F32),
            pltpu.VMEM((R, M), F32),
            pltpu.VMEM((2 * W, nz, R, Q), BF16),
            pltpu.VMEM((2 * W, nz, R, Q), BF16),
            pltpu.VMEM((2 * W, R, Q), F32),
            pltpu.VMEM((W, R, Q), BF16),
            pltpu.VMEM((W, R, Q), BF16),
            dma((CH,)),
            dma((W,)),
            dma((W,)),
            dma((2 * W, nz)),
            dma((2 * W, nz)),
            dma((W, CH)),
            dma((W, CH)),
            dma((2 * W, nz)),
            dma((2 * W, nz)),
            dma((W,)),
            dma((W,)),
        ],
        compiler_params=pltpu.CompilerParams(collective_id=0, has_side_effects=True, vmem_limit_bytes=60 << 20),
    )(chol_half, theta)


def on_device(mesh, chol_half, theta):
    G, R, M = chol_half.shape
    nz = mesh.shape["vec"]
    if mesh.shape["occ"] == 2 and R % 128 == 0 and theta.shape[1] % 128 == 0 and G * R * M <= 8 << 20:
        return fused(nz, chol_half, theta)
    widened = lax.all_gather(theta, "occ", axis=2, tiled=True)
    amplitude_sums = jnp.einsum(
        "gip,wpj->wgij", chol_half, lax.all_gather(widened, "vec", axis=1, tiled=True), preferred_element_type=F32
    )
    amplitudes = amplitude_sums.astype(BF16)
    swapped = lax.all_to_all(amplitudes, "occ", split_axis=3, concat_axis=2, tiled=True)
    summed_rows = lax.psum_scatter(
        jnp.einsum("gap,wgba->pwb", chol_half, swapped, preferred_element_type=F32),
        "vec",
        scatter_dimension=0,
        tiled=True,
    )
    owned = lax.psum_scatter(summed_rows, "occ", scatter_dimension=2, tiled=True)
    return -jnp.transpose(owned, (1, 0, 2))


def solution(mesh):
    return jax.shard_map(
        functools.partial(on_device, mesh),
        mesh=mesh,
        in_specs=(P(("grp", "vec"), "occ", None), P(("grp", "wlk"), "vec", "occ")),
        out_specs=P(("grp", "wlk"), "vec", "occ"),
        check_vma=False,
    )
```
